32 devices in a mesh: tm: 16 (over z, y, x), rep: 2 (over core).
Axes of the slice: x: 2, y: 2, z: 4, core: 2. Of those that a mesh axis runs over, the one named last changes fastest.
Arguments:
- rows: float32 [65536, 256], P('tm', 'rep'), may hold values from -90 to 90, as said below
- row_mask: int32 [65536], P('tm'), may hold values from 0 to 1, as said below
- key_bucket: int32 [65536], P('tm'), may hold values from 0 to 15
- gain: float32 [256], P('rep'), may hold values from 0.1 to 1.9
Outputs:
- keyed: float32 [49152, 256], P('tm', 'rep')
The draws below stay inside these ranges and needn't reach their ends.
Inputs may be any that keep to these rules, and one draw needn't show every extreme that they name: `rows`: scale per column differs; entries stay in the range. `row_mask`: of the 4096 rows of each index of tm, at least 2048 pass. Among the passing rows of one index of tm, no key bucket occurs more than 192 times, and one bucket, the same for all indices, occurs exactly 192 times on every index.
All inputs are finite; a program needn't handle non-finite values.
Results may differ from the reference program's by a relative error of at most 0.0003.
Values sent between devices are 32-bit elements; how exact they have to be, the bound alone decides.
A program may use at most 64 MiB of HBM per device.

```python
import math
import jax
import jax.numpy as jnp
from jax import lax

F = 256
WINDOW = 512
ROWS_DEV = 4096
TOTAL = 65536
MOST = 192
N_TM = 16


def draw_rows(key, part):
    kcol, kval = jax.random.split(jax.random.fold_in(key, 11), 2)
    column = jnp.exp(jax.random.uniform(kcol, (F,), jnp.float32, 0.0, math.log(10.0)))
    base = jnp.clip(jax.random.normal(kval, (TOTAL, F), jnp.float32), -6.0, 6.0)
    return base * column[None, :]


def mask_and_keys(key):
    base = jax.random.fold_in(key, 29)
    khot, kperm, kdev = jax.random.split(base, 3)
    hot = jax.random.randint(khot, (), 0, N_TM)
    relabel = jax.random.permutation(kperm, N_TM - 1).astype(jnp.int32)
    device_keys = jax.random.split(kdev, N_TM)

    def one_device(dkey):
        ka, kb, kc, kd, ke, kf, kg = jax.random.split(dkey, 7)
        places = jnp.arange(ROWS_DEV, dtype=jnp.int32)
        rate = jax.random.randint(ka, (), 0, 61)
        raw = jax.random.randint(kb, (ROWS_DEV,), 0, 100) < rate
        phase = jax.random.randint(kc, (), 0, 2)
        forced = places % 2 == phase
        start = jax.random.randint(kd, (), 0, ROWS_DEV - MOST + 1)
        inrun = (places >= start) & (places < start + MOST)
        offset = jax.random.randint(ke, (), 0, N_TM - 1)
        spread = (places // 2 + offset) % (N_TM - 1)
        picked = jnp.minimum(jax.random.randint(kf, (ROWS_DEV,), 0, N_TM - 1), jax.random.randint(kg, (ROWS_DEV,), 0, N_TM - 1))
        other = jnp.where(forced, spread, relabel[picked])
        bucket = jnp.where(other >= hot, other + 1, other)
        bucket = jnp.where(inrun, hot, bucket).astype(jnp.int32)
        live = inrun | forced | raw
        sortkey = jnp.where(live, bucket * 2 + jnp.where(inrun | forced, 0, 1), 2 * N_TM).astype(jnp.int32)
        order = jnp.argsort(sortkey, stable=True).astype(jnp.int32)
        ordered = sortkey[order]
        first = jnp.searchsorted(ordered, ordered // 2 * 2, side='left').astype(jnp.int32)
        rank = jnp.zeros((ROWS_DEV,), jnp.int32).at[order].set(places - first)
        keep = live & (rank < MOST)
        return (keep.astype(jnp.int32), bucket)
    masks, buckets = jax.vmap(one_device)(device_keys)
    return (masks.reshape(-1), buckets.reshape(-1))


def draw_row_mask(key, part):
    return mask_and_keys(key)[0]


def draw_key_bucket(key, part):
    return mask_and_keys(key)[1]


def setup_inputs(seed: int = 0) -> dict:
    key_list = jax.random.split(jax.random.key(seed), 5)
    rows = draw_rows(jax.random.fold_in(key_list[4], 71), 0)
    row_mask = draw_row_mask(jax.random.fold_in(key_list[4], 71), 0)
    key_bucket = draw_key_bucket(jax.random.fold_in(key_list[4], 71), 0)
    gain = jnp.clip(1.0 + 0.18 * jax.random.normal(key_list[3], (F,), jnp.float32), 0.1, 1.9)
    return {"rows": rows, "row_mask": row_mask, "key_bucket": key_bucket, "gain": gain}


epsilon = 1e-06

def window_sums(extended, width):
    blocks = extended.reshape(-1, width, extended.shape[1])
    inner = jnp.cumsum(blocks, axis=1)
    totals = inner[:, -1:, :]
    result = inner[1:] + totals[:-1] - inner[:-1]
    return result.reshape(-1, extended.shape[1])

def reference(rows, row_mask, key_bucket, gain):
    total_rows = rows.shape[0]
    capacity = N_TM * MOST
    positions = jnp.arange(total_rows, dtype=jnp.int32)
    live = row_mask == 1
    order_rank = (jnp.cumsum(row_mask) - 1).astype(jnp.int32)
    count = jnp.sum(row_mask).astype(jnp.int32)
    target = jnp.where(live, order_rank, total_rows).astype(jnp.int32)
    source = jnp.zeros((total_rows,), jnp.int32).at[target].set(positions, mode='drop')
    valid = positions < count
    compact = jnp.where(valid[:, None], rows[source], jnp.float32(0.0))
    compact_key = jnp.where(valid, key_bucket[source], N_TM).astype(jnp.int32)
    tail = lax.dynamic_slice_in_dim(compact, (count - WINDOW).astype(jnp.int32), WINDOW, 0)
    extended = jnp.concatenate([tail, compact], axis=0)
    sums = window_sums(extended, WINDOW)
    meansq = lax.optimization_barrier(jnp.mean(sums * sums, axis=1, keepdims=True))
    normed = sums * gain[None, :] / jnp.sqrt(meansq + epsilon)
    order = jnp.argsort(compact_key, stable=True).astype(jnp.int32)
    ordered = compact_key[order]
    first = jnp.searchsorted(ordered, ordered, side='left').astype(jnp.int32)
    placed = positions - first
    bucket_rank = jnp.zeros((total_rows,), jnp.int32).at[order].set(placed)
    dest = jnp.where(valid, compact_key * capacity + bucket_rank, N_TM * capacity).astype(jnp.int32)
    keyed = jnp.zeros((N_TM * capacity, rows.shape[1]), jnp.float32).at[dest].set(normed, mode='drop')
    return keyed
```

```python
import functools

import jax
import jax.numpy as jnp
from jax import lax
from jax.experimental import pallas as pl
from jax.experimental.pallas import tpu as pltpu
from jax.sharding import PartitionSpec as P

F = 256
WINDOW = 512
EPS = 1e-06
LANES = 128
STEP = 64
VMEM = pltpu.MemorySpace.VMEM
SMEM = pltpu.MemorySpace.SMEM
f32, bf16, i32 = jnp.float32, jnp.bfloat16, jnp.int32


def iota(shape, axis):
    return lax.broadcasted_iota(i32, shape, axis)


def dot(a, b):
    return jnp.dot(a, b, preferred_element_type=f32)


def compact_kernel(nodes, most, rows, mask, key, empty, packed, tail, source, counts,
                   place_v, slot_v, place_s, slot_s, sems):
    lines = mask.shape[0]
    slots = nodes * most
    fill = pltpu.make_async_copy(empty, source, sems.at[0])
    fill.start()
    one = jnp.ones((), f32)
    upper = (iota((LANES, LANES), 0) <= iota((LANES, LANES), 1)).astype(f32).astype(bf16)
    both = jnp.concatenate([upper, jnp.ones((LANES, LANES), bf16)], axis=0)
    group = min(nodes, 16)
    size = group * lines
    r, c = iota((size, size), 0), iota((size, size), 1)
    earlier = ((r // lines == c // lines) & (c < r)).astype(f32).astype(bf16)

    live = mask[...] == 1
    livef = live.astype(f32)
    keys = key[...]

    def prefix(hits, lower):
        hits = hits.astype(bf16)
        above = dot(lower, hits).astype(bf16)
        return dot(jnp.concatenate([hits, above], axis=1), both)

    place_v[...] = (prefix(livef, earlier[:lines, :lines]) - livef).astype(i32)
    slot = (one - livef) * slots
    lane = iota((8, LANES), 1)
    parts = []
    for first in range(0, nodes, group):
        hits = [(live & (keys == b)).astype(f32) for b in range(first, first + group)]
        running = prefix(jnp.concatenate(hits, axis=0), earlier)
        for j, hit in enumerate(hits):
            b = first + j
            mine = running[j * lines:(j + 1) * lines]
            slot = slot + hit * (mine + (b * most - 1.0))
            parts.append(jnp.where(lane == b % LANES, mine[lines - 1:lines, LANES - 1:LANES], 0.0))
    counts[...] = sum(parts)
    slot_v[...] = slot.astype(i32)
    c1 = pltpu.make_async_copy(place_v, place_s, sems.at[1])
    c2 = pltpu.make_async_copy(slot_v, slot_s, sems.at[2])
    c1.start()
    c2.start()
    fill.wait()
    c1.wait()
    c2.wait()

    def line(i, carry):
        def some(q, carry):
            for u in range(16):
                j = q * 16 + u
                g = place_s[i, j]
                packed[pl.ds(g, 1), :] = rows[pl.ds(i * LANES + j, 1), :]
                source[slot_s[i, j]] = g
            return carry
        return lax.fori_loop(0, LANES // 16, some, carry)

    lax.fori_loop(0, lines, line, 0)
    count = place_s[lines - 1, LANES - 1] + (slot_s[lines - 1, LANES - 1] < slots).astype(i32)
    tail[...] = packed[pl.ds(count - WINDOW, WINDOW), :]


def exchange_kernel(nodes, most, packed, tail, source, counts, gain, got, gotc,
                    tailbuf, w8, w64, sums, mine, other, send,
                    tsem, qsem, ssem, rsem, cssem, crsem):
    slots = nodes * most
    me, rep = lax.axis_index("tm"), lax.axis_index("rep")
    barrier = pltpu.get_barrier_semaphore()

    def hello(k, carry):
        pl.semaphore_signal(barrier, inc=1, device_id={"tm": lax.rem(me + k, nodes)})
        return carry

    lax.fori_loop(1, nodes, hello, 0)
    pl.semaphore_signal(barrier, inc=1, device_id={"rep": 1 - rep})
    pl.semaphore_wait(barrier, nodes)

    ahead = pltpu.make_async_remote_copy(
        src_ref=tail, dst_ref=tailbuf, send_sem=tsem.at[0], recv_sem=tsem.at[1],
        device_id={"tm": lax.rem(me + 1, nodes)})
    ahead.start()

    def count_copy(d, at):
        return pltpu.make_async_remote_copy(
            src_ref=counts, dst_ref=gotc.at[at], send_sem=cssem.at[d], recv_sem=crsem.at[at],
            device_id={"tm": d})

    def send_counts(k, carry):
        count_copy(lax.rem(me + k, nodes), me).start()
        return carry

    lax.fori_loop(1, nodes, send_counts, 0)
    gotc[me] = counts[...]

    def eight(x):
        x = x + pltpu.roll(x, 1, 0)
        x = x + pltpu.roll(x, 2, 0)
        x = x + pltpu.roll(x, 4, 0)
        return x[8:]

    def w8_own(c, carry):
        a = pl.multiple_of(c * STEP, STEP)
        w8[pl.ds(WINDOW + a, STEP), :] = eight(packed[pl.ds(a - 8, STEP + 8), :])
        return carry

    def stride_sum(ref, a, rows, stride):
        parts = [ref[pl.ds(a - stride * k, rows), :] for k in range(8)]
        while len(parts) > 1:
            parts = [parts[i] + parts[i + 1] for i in range(0, len(parts), 2)]
        return parts[0]

    def w64_at(c, carry):
        a = pl.multiple_of(c * STEP, STEP)
        w64[pl.ds(a, STEP), :] = stride_sum(w8, a, STEP, 8)
        return carry

    ones = jnp.ones((8, LANES), f32)

    def w512_at(c, carry):
        a = pl.multiple_of(c * LANES, LANES)
        total = stride_sum(w64, WINDOW + a, LANES, 64)
        sums[pl.ds(a, LANES), :] = total
        sq = lax.dot_general(ones, total * total, (((1,), (1,)), ((), ())),
                             precision=lax.Precision.HIGHEST, preferred_element_type=f32)
        mine[pl.ds(c, 1), :] = sq[0:1]
        return carry

    own = WINDOW // STEP + 1
    last = (WINDOW + slots) // STEP
    lax.fori_loop(1, slots // STEP, w8_own, 0)
    lax.fori_loop(own + 1, last, w64_at, 0)
    lax.fori_loop(5, slots // LANES, w512_at, 0)
    ahead.wait()
    w8[0:STEP, :] = eight(jnp.concatenate([jnp.zeros((8, LANES), f32), tailbuf[0:STEP, :]], axis=0))
    for a in range(STEP, WINDOW, STEP):
        w8[a:a + STEP, :] = eight(tailbuf[a - 8:a + STEP, :])
    w8[WINDOW:WINDOW + STEP, :] = eight(
        jnp.concatenate([tailbuf[WINDOW - 8:WINDOW, :], packed[0:STEP, :]], axis=0))
    lax.fori_loop(1, own + 1, w64_at, 0)
    lax.fori_loop(0, 5, w512_at, 0)

    swap = pltpu.make_async_remote_copy(
        src_ref=mine, dst_ref=other, send_sem=qsem.at[0], recv_sem=qsem.at[1],
        device_id={"rep": 1 - rep})
    swap.start()
    sums[pl.ds(slots, 8), :] = jnp.zeros((8, LANES), f32)
    swap.wait()

    gains = gain[...]

    def scale(c, carry):
        a = pl.multiple_of(c * LANES, LANES)
        full = mine[pl.ds(c, 1), :] + other[pl.ds(c, 1), :]
        inv = lax.rsqrt(full / F + EPS)
        column = jnp.broadcast_to(inv, (LANES, LANES)).T
        sums[pl.ds(a, LANES), :] = sums[pl.ds(a, LANES), :] * gains * column
        return carry

    lax.fori_loop(0, slots // LANES, scale, 0)

    def gather(ref, d):
        def some(q, carry):
            for u in range(8):
                j = q * 8 + u
                ref[d, pl.ds(j, 1), :] = sums[pl.ds(source[d * most + j], 1), :]
            return carry
        lax.fori_loop(0, most // 8, some, 0)

    def block_copy(d, at):
        return pltpu.make_async_remote_copy(
            src_ref=send.at[d], dst_ref=got.at[at], send_sem=ssem.at[d], recv_sem=rsem.at[at],
            device_id={"tm": d})

    def send_block(k, carry):
        d = lax.rem(me + k, nodes)
        gather(send, d)
        block_copy(d, me).start()
        return carry

    lax.fori_loop(1, nodes, send_block, 0)
    gather(got, me)

    def finish(k, carry):
        s = lax.rem(me + k, nodes)
        count_copy(s, s).wait()
        block_copy(s, s).wait()
        return carry

    lax.fori_loop(1, nodes, finish, 0)


def place_kernel(nodes, most, got, gotc, out):
    me = lax.axis_index("tm")
    out[...] = jnp.zeros_like(out)
    lane = iota((1, LANES), 1)

    def sender(s, start):
        out[pl.ds(start, most), :] = got[s]
        number = jnp.sum(jnp.where(lane == me, gotc[s, 0:1, :], 0.0))
        return start + number.astype(i32)

    lax.fori_loop(0, nodes, sender, jnp.int32(0))


def local(nodes, rows, row_mask, key_bucket, gain):
    size_rows, half = rows.shape
    most = 3 * size_rows // (4 * nodes)
    slots = nodes * most
    lines = size_rows // LANES
    vm = pl.BlockSpec(memory_space=VMEM)
    sm = pl.BlockSpec(memory_space=SMEM)
    hbm = pl.BlockSpec(memory_space=pl.ANY)
    empty = jnp.full((slots + LANES,), slots, i32)
    packed, tail, source, counts = pl.pallas_call(
        functools.partial(compact_kernel, nodes, most),
        out_shape=(
            jax.ShapeDtypeStruct((slots + 8, half), f32),
            jax.ShapeDtypeStruct((WINDOW, half), f32),
            jax.ShapeDtypeStruct((slots + LANES,), i32),
            jax.ShapeDtypeStruct((8, LANES), f32),
        ),
        in_specs=[vm, vm, vm, hbm],
        out_specs=(vm, vm, sm, vm),
        scratch_shapes=[
            pltpu.VMEM((lines, LANES), i32),
            pltpu.VMEM((lines, LANES), i32),
            pltpu.SMEM((lines, LANES), i32),
            pltpu.SMEM((lines, LANES), i32),
            pltpu.SemaphoreType.DMA((3,)),
        ],
        name="compact",
    )(rows, row_mask.reshape(lines, LANES), key_bucket.reshape(lines, LANES), empty)
    dma = pltpu.SemaphoreType.DMA
    got, gotc = pl.pallas_call(
        functools.partial(exchange_kernel, nodes, most),
        out_shape=(
            jax.ShapeDtypeStruct((nodes, most, half), f32),
            jax.ShapeDtypeStruct((nodes, 8, LANES), f32),
        ),
        in_specs=[vm, vm, sm, vm, vm],
        out_specs=(vm, vm),
        scratch_shapes=[
            pltpu.VMEM((WINDOW, half), f32),
            pltpu.VMEM((WINDOW + slots, half), f32),
            pltpu.VMEM((WINDOW + slots, half), f32),
            pltpu.VMEM((slots + 8, half), f32),
            pltpu.VMEM((slots // LANES, LANES), f32),
            pltpu.VMEM((slots // LANES, LANES), f32),
            pltpu.VMEM((nodes, most, half), f32),
            dma((2,)), dma((2,)), dma((nodes,)), dma((nodes,)), dma((nodes,)), dma((nodes,)),
        ],
        compiler_params=pltpu.CompilerParams(collective_id=0, has_side_effects=True),
        name="exchange",
    )(packed, tail, source, counts, gain.reshape(1, half))
    return pl.pallas_call(
        functools.partial(place_kernel, nodes, most),
        out_shape=jax.ShapeDtypeStruct((slots, half), f32),
        in_specs=[vm, vm],
        out_specs=vm,
        name="place",
    )(got, gotc)


def solution(mesh):
    in_specs = (P("tm", "rep"), P("tm"), P("tm"), P("rep"))
    body = functools.partial(local, mesh.shape["tm"])
    return jax.shard_map(body, mesh=mesh, in_specs=in_specs, out_specs=P("tm", "rep"), check_vma=False)
```

```python
import functools

import jax
import jax.numpy as jnp
from jax import lax
from jax.experimental import pallas as pl
from jax.experimental.pallas import tpu as pltpu
from jax.sharding import PartitionSpec as P

F = 256
WINDOW = 512
EPS = 1e-06
LANES = 128
STEP = 64
VMEM = pltpu.MemorySpace.VMEM
SMEM = pltpu.MemorySpace.SMEM
f32, bf16, i32 = jnp.float32, jnp.bfloat16, jnp.int32


def iota(shape, axis):
    return lax.broadcasted_iota(i32, shape, axis)


def dot(a, b):
    return jnp.dot(a, b, preferred_element_type=f32)


def compact_kernel(nodes, most, rows, mask, key, packed, tail, source, counts,
                   running_v, within_v, piece_v, column_v, value_v, running_s, sem):
    lines = mask.shape[0]
    slots = nodes * most
    upper = (iota((LANES, LANES), 0) <= iota((LANES, LANES), 1)).astype(f32).astype(bf16)
    both = jnp.concatenate([upper, jnp.ones((LANES, LANES), bf16)], axis=0)
    group = min(nodes, 16)
    size = group * lines
    r, c = iota((size, size), 0), iota((size, size), 1)
    earlier = ((r // lines == c // lines) & (c < r)).astype(f32).astype(bf16)

    live = mask[...] == 1
    livef = live.astype(f32)
    keys = key[...]

    def prefix(hits, lower):
        hits = hits.astype(bf16)
        above = dot(lower, hits).astype(bf16)
        return dot(jnp.concatenate([hits, above], axis=1), both)

    running = prefix(livef, earlier[:lines, :lines])
    running_v[...] = running.astype(i32)
    fetch = pltpu.make_async_copy(running_v, running_s, sem)
    fetch.start()
    within = dot(livef.astype(bf16), upper).astype(i32) - 1
    within_v[...] = jnp.where(live, within, -1)
    slot = jnp.zeros((lines, LANES), f32)
    lane = iota((8, LANES), 1)
    parts = []
    for first in range(0, nodes, group):
        hits = [(live & (keys == b)).astype(f32) for b in range(first, first + group)]
        ranks = prefix(jnp.concatenate(hits, axis=0), earlier)
        for j, hit in enumerate(hits):
            b = first + j
            mine = ranks[j * lines:(j + 1) * lines]
            slot = slot + hit * (mine + (b * most - 1.0))
            parts.append(jnp.where(lane == b % LANES, mine[lines - 1:lines, LANES - 1:LANES], 0.0))
    counts[...] = sum(parts)
    slot = slot.astype(i32)
    piece_v[...] = jnp.where(live, slot // LANES, -1)
    column_v[...] = slot % LANES
    value_v[...] = slots + 1 - running.astype(i32)

    pieces = slots // LANES
    down = iota((LANES, LANES), 0)
    piece_down = iota((pieces, LANES), 0)
    each = 4

    def invert(q, total):
        for u in range(each):
            at = pl.ds(q * each + u, 1)
            value = value_v[at, :]
            hit = piece_down == piece_v[at, :]
            high = jnp.where(hit, (value // LANES).astype(f32), 0.0)
            low = jnp.where(hit, (value % LANES).astype(f32), 0.0)
            left = jnp.concatenate([high, low], axis=0).astype(bf16)
            right = (down == column_v[at, :]).astype(f32).astype(bf16)
            total = total + lax.dot_general(
                left, right, (((1,), (1,)), ((), ())), preferred_element_type=f32)
        return total

    total = lax.fori_loop(0, lines // each, invert, jnp.zeros((2 * pieces, LANES), f32))
    source[...] = slots - (total[:pieces] * LANES + total[pieces:]).astype(i32)
    fetch.wait()

    def pack(q, start):
        for u in range(each):
            i = q * each + u
            pick = (down == within_v[pl.ds(i, 1), :]).astype(f32).astype(bf16)
            x = rows[pl.ds(pl.multiple_of(i * LANES, LANES), LANES), :]
            high = x.astype(bf16)
            rest = x - high.astype(f32)
            middle = rest.astype(bf16)
            low = (rest - middle.astype(f32)).astype(bf16)
            got = dot(pick, jnp.concatenate([high, middle, low], axis=1))
            packed[pl.ds(start, LANES), :] = (
                got[:, :LANES] + (got[:, LANES:2 * LANES] + got[:, 2 * LANES:]))
            start = running_s[i, LANES - 1]
        return start

    count = lax.fori_loop(0, lines // each, pack, jnp.int32(0))
    tail[...] = packed[pl.ds(count - WINDOW, WINDOW), :]


def exchange_kernel(nodes, most, packed, tail, source, counts, gain, out, gotc,
                    tailbuf, w8, w64, sums, mine, other, send, got,
                    tsem, qssem, qrsem, ssem, rsem, cssem, crsem, osem):
    slots = nodes * most
    me, rep = lax.axis_index("tm"), lax.axis_index("rep")
    barrier = pltpu.get_barrier_semaphore()

    def hello(k, carry):
        pl.semaphore_signal(barrier, inc=1, device_id={"tm": lax.rem(me + k, nodes)})
        return carry

    lax.fori_loop(1, nodes, hello, 0)
    pl.semaphore_signal(barrier, inc=1, device_id={"rep": 1 - rep})
    pl.semaphore_wait(barrier, nodes)

    ahead = pltpu.make_async_remote_copy(
        src_ref=tail, dst_ref=tailbuf, send_sem=tsem.at[0], recv_sem=tsem.at[1],
        device_id={"tm": lax.rem(me + 1, nodes)})
    ahead.start()

    def count_copy(d, at):
        return pltpu.make_async_remote_copy(
            src_ref=counts, dst_ref=gotc.at[at], send_sem=cssem.at[d], recv_sem=crsem.at[at],
            device_id={"tm": d})

    def send_counts(k, carry):
        count_copy(lax.rem(me + k, nodes), me).start()
        return carry

    lax.fori_loop(1, nodes, send_counts, 0)
    gotc[me] = counts[...]

    def eight(x):
        x = x + pltpu.roll(x, 1, 0)
        x = x + pltpu.roll(x, 2, 0)
        x = x + pltpu.roll(x, 4, 0)
        return x[8:]

    def w8_own(c, carry):
        a = pl.multiple_of(c * STEP, STEP)
        w8[pl.ds(WINDOW + a, STEP), :] = eight(packed[pl.ds(a - 8, STEP + 8), :])
        return carry

    def stride_sum(ref, a, rows, stride):
        parts = [ref[pl.ds(a - stride * k, rows), :] for k in range(8)]
        while len(parts) > 1:
            parts = [parts[i] + parts[i + 1] for i in range(0, len(parts), 2)]
        return parts[0]

    def w64_at(c, carry):
        a = pl.multiple_of(c * STEP, STEP)
        w64[pl.ds(a, STEP), :] = stride_sum(w8, a, STEP, 8)
        return carry

    def w512_at(c, carry):
        a = pl.multiple_of(c * LANES, LANES)
        sums[pl.ds(a, LANES), :] = stride_sum(w64, WINDOW + a, LANES, 64)
        return carry

    own = WINDOW // STEP + 1
    last = (WINDOW + slots) // STEP
    lax.fori_loop(1, slots // STEP, w8_own, 0)
    lax.fori_loop(own + 1, last, w64_at, 0)
    lax.fori_loop(5, slots // LANES, w512_at, 0)
    ahead.wait()
    w8[0:STEP, :] = eight(jnp.concatenate([jnp.zeros((8, LANES), f32), tailbuf[0:STEP, :]], axis=0))
    for a in range(STEP, WINDOW, STEP):
        w8[a:a + STEP, :] = eight(tailbuf[a - 8:a + STEP, :])
    w8[WINDOW:WINDOW + STEP, :] = eight(
        jnp.concatenate([tailbuf[WINDOW - 8:WINDOW, :], packed[0:STEP, :]], axis=0))
    lax.fori_loop(1, own + 1, w64_at, 0)
    lax.fori_loop(0, 5, w512_at, 0)

    sums[pl.ds(slots, 8), :] = jnp.zeros((8, LANES), f32)

    def gather(ref, d):
        def some(q, carry):
            for u in range(8):
                j = q * 8 + u
                ref[d, pl.ds(j, 1), :] = sums[pl.ds(source[d * most + j], 1), :]
            return carry
        lax.fori_loop(0, most // 8, some, 0)

    def block_copy(d, at):
        return pltpu.make_async_remote_copy(
            src_ref=send.at[d], dst_ref=got.at[at], send_sem=ssem.at[d], recv_sem=rsem.at[at],
            device_id={"tm": d})

    half = nodes // 2
    near, far = me // half * half, (me // half + 1) % 2 * half
    seat = me % half

    def send_block(base, k):
        d = base + (seat + k) % half
        gather(send, d)
        block_copy(d, me).start()

    def swap_copy(s):
        return pltpu.make_async_remote_copy(
            src_ref=mine.at[s], dst_ref=other.at[s], send_sem=qssem.at[s], recv_sem=qrsem.at[s],
            device_id={"rep": 1 - rep})

    def out_copy(s):
        return pltpu.make_async_copy(got.at[s], out.at[s], osem.at[s])

    def squares(s):
        x = got[s]
        mine[s] = jnp.broadcast_to(jnp.sum(x * x, axis=1, keepdims=True), x.shape)
        swap_copy(s).start()

    gains = gain[...]

    def norm(s):
        swap_copy(s).wait()
        got[s] = got[s] * gains * lax.rsqrt((mine[s] + other[s]) / F + EPS)
        out_copy(s).start()

    def receive(base, k):
        s = base + (seat + half - k) % half
        block_copy(s, s).wait()
        squares(s)
        return s

    def loop(first, last, body, carry):
        return lax.fori_loop(first, last, body, carry)

    def send_far(k, carry):
        send_block(far, k)
        return carry

    def send_near(k, carry):
        send_block(near, k)
        return carry

    loop(0, half, send_far, 0)
    loop(1, half, send_near, 0)
    gather(got, me)
    squares(me)

    def get_far(k, carry):
        receive(far, k)
        before = jnp.where(k == 0, me, far + (seat + half - k + 1) % half)
        norm(before)
        return carry

    def get_near(k, carry):
        receive(near, k)
        before = jnp.where(k == 1, far + (seat + 1) % half, near + (seat + half - k + 1) % half)
        norm(before)
        return carry

    loop(0, half, get_far, 0)
    loop(1, half, get_near, 0)
    norm(near + (seat + 1) % half)

    def finish(k, carry):
        s = lax.rem(me + k, nodes)
        count_copy(s, s).wait()
        return carry

    loop(1, nodes, finish, 0)

    def left(s, carry):
        out_copy(s).wait()
        return carry

    loop(0, nodes, left, 0)


def place_kernel(nodes, most, got, gotc, out):
    me = lax.axis_index("tm")
    out[...] = jnp.zeros_like(out)
    lane = iota((1, LANES), 1)

    def sender(s, start):
        out[pl.ds(start, most), :] = got[s]
        number = jnp.sum(jnp.where(lane == me, gotc[s, 0:1, :], 0.0))
        return start + number.astype(i32)

    lax.fori_loop(0, nodes, sender, jnp.int32(0))


def local(nodes, rows, row_mask, key_bucket, gain):
    size_rows, half = rows.shape
    most = 3 * size_rows // (4 * nodes)
    slots = nodes * most
    lines = size_rows // LANES
    vm = pl.BlockSpec(memory_space=VMEM)
    sm = pl.BlockSpec(memory_space=SMEM)
    hbm = pl.BlockSpec(memory_space=pl.ANY)
    table = pltpu.VMEM((lines, LANES), i32)
    packed, tail, source, counts = pl.pallas_call(
        functools.partial(compact_kernel, nodes, most),
        out_shape=(
            jax.ShapeDtypeStruct((slots + LANES, half), f32),
            jax.ShapeDtypeStruct((WINDOW, half), f32),
            jax.ShapeDtypeStruct((slots // LANES, LANES), i32),
            jax.ShapeDtypeStruct((8, LANES), f32),
        ),
        in_specs=[vm, vm, vm],
        out_specs=(vm, vm, vm, vm),
        scratch_shapes=[
            table, table, table, table, table,
            pltpu.SMEM((lines, LANES), i32),
            pltpu.SemaphoreType.DMA,
        ],
        name="compact",
    )(rows, row_mask.reshape(lines, LANES), key_bucket.reshape(lines, LANES))
    source = source.reshape(slots)
    dma = pltpu.SemaphoreType.DMA
    blocks = pltpu.VMEM((nodes, most, half), f32)
    got, gotc = pl.pallas_call(
        functools.partial(exchange_kernel, nodes, most),
        out_shape=(
            jax.ShapeDtypeStruct((nodes, most, half), f32),
            jax.ShapeDtypeStruct((nodes, 8, LANES), f32),
        ),
        in_specs=[vm, vm, sm, vm, vm],
        out_specs=(hbm, vm),
        scratch_shapes=[
            pltpu.VMEM((WINDOW, half), f32),
            pltpu.VMEM((WINDOW + slots, half), f32),
            pltpu.VMEM((WINDOW + slots, half), f32),
            pltpu.VMEM((slots + 8, half), f32),
            blocks, blocks, blocks, blocks,
            dma((2,)),
        ] + [dma((nodes,))] * 7,
        compiler_params=pltpu.CompilerParams(collective_id=0, has_side_effects=True),
        name="exchange",
    )(packed, tail, source, counts, gain.reshape(1, half))
    return pl.pallas_call(
        functools.partial(place_kernel, nodes, most),
        out_shape=jax.ShapeDtypeStruct((slots, half), f32),
        in_specs=[vm, vm],
        out_specs=vm,
        name="place",
    )(got, gotc)


def solution(mesh):
    in_specs = (P("tm", "rep"), P("tm"), P("tm"), P("rep"))
    body = functools.partial(local, mesh.shape["tm"])
    return jax.shard_map(body, mesh=mesh, in_specs=in_specs, out_specs=P("tm", "rep"), check_vma=False)
```

```python
import functools

import jax
import jax.numpy as jnp
from jax import lax
from jax.experimental import pallas as pl
from jax.experimental.pallas import tpu as pltpu
from jax.sharding import PartitionSpec as P

F = 256
WINDOW = 512
EPS = 1e-06
LANES = 128
STEP = 64
VMEM = pltpu.MemorySpace.VMEM
SMEM = pltpu.MemorySpace.SMEM
f32, bf16, i32 = jnp.float32, jnp.bfloat16, jnp.int32


def iota(shape, axis):
    return lax.broadcasted_iota(i32, shape, axis)


def within(x, low, high):
    return jnp.minimum(jnp.maximum(x, low), high)


def dot(a, b):
    return jnp.dot(a, b, preferred_element_type=f32)


def exchange_kernel(nodes, most, wide, rows_hbm, mask, key, gain, out, gotc,
                    rows, packed, tail, tailbuf, w8, w64, sums, mine, other, send, got, counts,
                    order_v, source_v, first_v, second_v, order_s, source_s,
                    lsem, tsem, qssem, qrsem, ssem, rsem, cssem, crsem, osem):
    slots = nodes * most
    lines = mask.shape[0]
    me, rep = lax.axis_index("tm"), lax.axis_index("rep")
    fetch = pltpu.make_async_copy(rows_hbm, rows, lsem.at[0])
    fetch.start()
    barrier = pltpu.get_barrier_semaphore()

    def hello(k, carry):
        pl.semaphore_signal(barrier, inc=1, device_id={"tm": lax.rem(me + k, nodes)})
        return carry

    lax.fori_loop(1, nodes, hello, 0)
    pl.semaphore_signal(barrier, inc=1, device_id={"rep": 1 - rep})

    upper = (iota((LANES, LANES), 0) <= iota((LANES, LANES), 1)).astype(f32).astype(bf16)
    both = jnp.concatenate([upper, jnp.ones((LANES, LANES), bf16)], axis=0)
    group = min(nodes, 16)
    size = group * lines
    r, c = iota((size, size), 0), iota((size, size), 1)
    earlier = ((r // lines == c // lines) & (c < r)).astype(f32).astype(bf16)
    live = mask[...] == 1
    livef = live.astype(f32)
    keys = key[...]

    def prefix(hits, lower):
        hits = hits.astype(bf16)
        above = dot(lower, hits).astype(bf16)
        return dot(jnp.concatenate([hits, above], axis=1), both)

    down = iota((LANES, LANES), 0)
    each = 4

    def invert(pieces, spot, values):
        first_v[...] = jnp.where(live, spot // LANES, -1)
        second_v[...] = spot % LANES
        piece_down = iota((pieces, LANES), 0)

        def some(q, total):
            for u in range(each):
                i = q * each + u
                high, low = values(i)
                hit = piece_down == first_v[pl.ds(i, 1), :]
                left = jnp.concatenate(
                    [jnp.where(hit, high, 0.0), jnp.where(hit, low, 0.0)], axis=0).astype(bf16)
                right = (down == second_v[pl.ds(i, 1), :]).astype(f32).astype(bf16)
                total = total + lax.dot_general(
                    left, right, (((1,), (1,)), ((), ())), preferred_element_type=f32)
            return total

        total = lax.fori_loop(0, lines // each, some, jnp.zeros((2 * pieces, LANES), f32))
        return (total[:pieces] * LANES + total[pieces:]).astype(i32)

    running = prefix(livef, earlier[:lines, :lines])
    place = running.astype(i32) - 1
    pieces = slots // LANES
    lanef = iota((1, LANES), 1).astype(f32)
    order_v[0:pieces, :] = within(invert(
        pieces, place, lambda i: (jnp.asarray(i, i32).astype(f32), lanef)), 0, lines * LANES - 1)
    order_v[pieces:pieces + 8, :] = within(jnp.broadcast_to(
        running[lines - 1:lines, LANES - 1:LANES], (8, LANES)).astype(i32), WINDOW, slots)
    list_copy = pltpu.make_async_copy(order_v, order_s, lsem.at[1])
    list_copy.start()
    list_copy.wait()
    fetch.wait()
    begin = order_s[pieces, 0] - WINDOW

    def take_tail(q, carry):
        for u in range(16):
            j = q * 16 + u
            g = begin + j
            tail[pl.ds(j, 1), :] = rows[pl.ds(order_s[g >> 7, g & (LANES - 1)], 1), :]
        return carry

    lax.fori_loop(0, WINDOW // 16, take_tail, 0)
    pl.semaphore_wait(barrier, nodes)
    ahead = pltpu.make_async_remote_copy(
        src_ref=tail, dst_ref=tailbuf, send_sem=tsem.at[0], recv_sem=tsem.at[1],
        device_id={"tm": lax.rem(me + 1, nodes)})
    ahead.start()

    slot = jnp.zeros((lines, LANES), f32)
    lane = iota((8, LANES), 1)
    parts = []
    for first in range(0, nodes, group):
        hits = [(live & (keys == b)).astype(f32) for b in range(first, first + group)]
        ranks = prefix(jnp.concatenate(hits, axis=0), earlier)
        for j, hit in enumerate(hits):
            b = first + j
            own = ranks[j * lines:(j + 1) * lines]
            slot = slot + hit * (own + (b * wide - 1.0))
            parts.append(jnp.where(lane == b % LANES, own[lines - 1:lines, LANES - 1:LANES], 0.0))
    counts[...] = sum(parts)
    back = slots - place
    packed[0:lines, :] = (back // LANES).astype(f32)
    packed[lines:2 * lines, :] = (back % LANES).astype(f32)
    source_v[...] = within(slots - invert(
        nodes * wide // LANES, slot.astype(i32),
        lambda i: (packed[pl.ds(i, 1), :], packed[pl.ds(lines + i, 1), :])), 0, slots)
    source_copy = pltpu.make_async_copy(source_v, source_s, lsem.at[2])
    source_copy.start()

    def count_copy(d, at):
        return pltpu.make_async_remote_copy(
            src_ref=counts, dst_ref=gotc.at[at], send_sem=cssem.at[d], recv_sem=crsem.at[at],
            device_id={"tm": d})

    def take(i, carry):
        def some(q, carry):
            for u in range(16):
                j = q * 16 + u
                packed[pl.ds(i * LANES + j, 1), :] = rows[pl.ds(order_s[i, j], 1), :]
            return carry
        return lax.fori_loop(0, LANES // 16, some, carry)

    lax.fori_loop(0, pieces, take, 0)

    def eight(x):
        x = x + pltpu.roll(x, 1, 0)
        x = x + pltpu.roll(x, 2, 0)
        x = x + pltpu.roll(x, 4, 0)
        return x[8:]

    def w8_own(c, carry):
        a = pl.multiple_of(c * STEP, STEP)
        w8[pl.ds(WINDOW + a, STEP), :] = eight(packed[pl.ds(a - 8, STEP + 8), :])
        return carry

    def stride_sum(ref, a, rows, stride):
        parts = [ref[pl.ds(a - stride * k, rows), :] for k in range(8)]
        while len(parts) > 1:
            parts = [parts[i] + parts[i + 1] for i in range(0, len(parts), 2)]
        return parts[0]

    def w64_at(c, carry):
        a = pl.multiple_of(c * STEP, STEP)
        w64[pl.ds(a, STEP), :] = stride_sum(w8, a, STEP, 8)
        return carry

    def w512_at(c, carry):
        a = pl.multiple_of(c * LANES, LANES)
        sums[pl.ds(a, LANES), :] = stride_sum(w64, WINDOW + a, LANES, 64)
        return carry

    own = WINDOW // STEP + 1
    last = (WINDOW + slots) // STEP
    lax.fori_loop(1, slots // STEP, w8_own, 0)
    lax.fori_loop(own + 1, last, w64_at, 0)
    lax.fori_loop(5, slots // LANES, w512_at, 0)
    ahead.wait()
    w8[0:STEP, :] = eight(jnp.concatenate([jnp.zeros((8, LANES), f32), tailbuf[0:STEP, :]], axis=0))
    for a in range(STEP, WINDOW, STEP):
        w8[a:a + STEP, :] = eight(tailbuf[a - 8:a + STEP, :])
    w8[WINDOW:WINDOW + STEP, :] = eight(
        jnp.concatenate([tailbuf[WINDOW - 8:WINDOW, :], packed[0:STEP, :]], axis=0))
    lax.fori_loop(1, own + 1, w64_at, 0)
    lax.fori_loop(0, 5, w512_at, 0)

    sums[pl.ds(slots, 8), :] = jnp.zeros((8, LANES), f32)

    def gather(ref, d):
        def some(q, carry):
            for u in range(8):
                j = q * 8 + u
                at = source_s[d * (wide // LANES) + q // (LANES // 8), q % (LANES // 8) * 8 + u]
                ref[d, pl.ds(j, 1), :] = sums[pl.ds(at, 1), :]
            return carry
        lax.fori_loop(0, most // 8, some, 0)

    def block_copy(d, at):
        return pltpu.make_async_remote_copy(
            src_ref=send.at[d], dst_ref=got.at[at], send_sem=ssem.at[d], recv_sem=rsem.at[at],
            device_id={"tm": d})

    half = nodes // 2
    near, far = me // half * half, (me // half + 1) % 2 * half
    seat = me % half

    def send_block(base, k):
        d = base + (seat + k) % half
        gather(send, d)
        block_copy(d, me).start()

    def swap_copy(s):
        return pltpu.make_async_remote_copy(
            src_ref=mine.at[s], dst_ref=other.at[s], send_sem=qssem.at[s], recv_sem=qrsem.at[s],
            device_id={"rep": 1 - rep})

    def out_copy(s):
        return pltpu.make_async_copy(got.at[s], out.at[s], osem.at[s])

    def squares(s):
        x = got[s]
        mine[s] = jnp.broadcast_to(jnp.sum(x * x, axis=1, keepdims=True), x.shape)
        swap_copy(s).start()

    gains = gain[...]

    def norm(s):
        swap_copy(s).wait()
        got[s] = got[s] * gains * lax.rsqrt((mine[s] + other[s]) / F + EPS)
        out_copy(s).start()

    def receive(base, k):
        s = base + (seat + half - k) % half
        block_copy(s, s).wait()
        squares(s)
        return s

    def loop(first, last, body, carry):
        return lax.fori_loop(first, last, body, carry)

    def send_far(k, carry):
        send_block(far, k)
        return carry

    def send_near(k, carry):
        send_block(near, k)
        return carry

    source_copy.wait()
    loop(0, half, send_far, 0)
    loop(1, half, send_near, 0)

    def send_counts(k, carry):
        count_copy(lax.rem(me + k, nodes), me).start()
        return carry

    loop(1, nodes, send_counts, 0)
    gotc[me] = counts[...]
    gather(got, me)
    squares(me)

    def get_far(k, carry):
        receive(far, k)
        before = jnp.where(k == 0, me, far + (seat + half - k + 1) % half)
        norm(before)
        return carry

    def get_near(k, carry):
        receive(near, k)
        before = jnp.where(k == 1, far + (seat + 1) % half, near + (seat + half - k + 1) % half)
        norm(before)
        return carry

    loop(0, half, get_far, 0)
    loop(1, half, get_near, 0)
    norm(near + (seat + 1) % half)

    def finish(k, carry):
        s = lax.rem(me + k, nodes)
        count_copy(s, s).wait()
        return carry

    loop(1, nodes, finish, 0)

    def left(s, carry):
        out_copy(s).wait()
        return carry

    loop(0, nodes, left, 0)


def place_kernel(nodes, most, got, gotc, out):
    me = lax.axis_index("tm")
    out[...] = jnp.zeros_like(out)
    lane = iota((1, LANES), 1)

    def sender(s, start):
        out[pl.ds(start, most), :] = got[s]
        number = jnp.sum(jnp.where(lane == me, gotc[s, 0:1, :], 0.0))
        return start + number.astype(i32)

    lax.fori_loop(0, nodes, sender, jnp.int32(0))


def local(nodes, rows, row_mask, key_bucket, gain):
    size_rows, half = rows.shape
    most = 3 * size_rows // (4 * nodes)
    slots = nodes * most
    lines = size_rows // LANES
    vm = pl.BlockSpec(memory_space=VMEM)
    hbm = pl.BlockSpec(memory_space=pl.ANY)
    wide = -(-most // LANES) * LANES
    dma = pltpu.SemaphoreType.DMA
    blocks = pltpu.VMEM((nodes, most, half), f32)
    edge = pltpu.VMEM((WINDOW, half), f32)
    table = pltpu.VMEM((lines, LANES), i32)
    order, source = (slots // LANES + 8, LANES), (nodes * wide // LANES, LANES)
    got, gotc = pl.pallas_call(
        functools.partial(exchange_kernel, nodes, most, wide),
        out_shape=(
            jax.ShapeDtypeStruct((nodes, most, half), f32),
            jax.ShapeDtypeStruct((nodes, 8, LANES), f32),
        ),
        in_specs=[hbm, vm, vm, vm],
        out_specs=(hbm, vm),
        scratch_shapes=[
            pltpu.VMEM((size_rows, half), f32),
            pltpu.VMEM((slots, half), f32),
            edge, edge,
            pltpu.VMEM((WINDOW + slots, half), f32),
            pltpu.VMEM((WINDOW + slots, half), f32),
            pltpu.VMEM((slots + 8, half), f32),
            blocks, blocks, blocks, blocks,
            pltpu.VMEM((8, LANES), f32),
            pltpu.VMEM(order, i32), pltpu.VMEM(source, i32),
            table, table,
            pltpu.SMEM(order, i32), pltpu.SMEM(source, i32),
            dma((3,)), dma((2,)),
        ] + [dma((nodes,))] * 7,
        compiler_params=pltpu.CompilerParams(collective_id=0, has_side_effects=True),
        name="exchange",
    )(rows, row_mask.reshape(lines, LANES), key_bucket.reshape(lines, LANES), gain.reshape(1, half))
    return pl.pallas_call(
        functools.partial(place_kernel, nodes, most),
        out_shape=jax.ShapeDtypeStruct((slots, half), f32),
        in_specs=[vm, vm],
        out_specs=vm,
        name="place",
    )(got, gotc)


def solution(mesh):
    in_specs = (P("tm", "rep"), P("tm"), P("tm"), P("rep"))
    body = functools.partial(local, mesh.shape["tm"])
    return jax.shard_map(body, mesh=mesh, in_specs=in_specs, out_specs=P("tm", "rep"), check_vma=False)
```

```python
import functools

import jax
import jax.numpy as jnp
from jax import lax
from jax.experimental import pallas as pl
from jax.experimental.pallas import tpu as pltpu
from jax.sharding import PartitionSpec as P

F = 256
WINDOW = 512
EPS = 1e-06
LANES = 128
STEP = 64
VMEM = pltpu.MemorySpace.VMEM
SMEM = pltpu.MemorySpace.SMEM
f32, bf16, i32 = jnp.float32, jnp.bfloat16, jnp.int32


def iota(shape, axis):
    return lax.broadcasted_iota(i32, shape, axis)


def within(x, low, high):
    return jnp.minimum(jnp.maximum(x, low), high)


def dot(a, b):
    return jnp.dot(a, b, preferred_element_type=f32)


def exchange_kernel(nodes, most, wide, rows_hbm, mask, key, gain, out, gotc,
                    rows, packed, tail, tailbuf, w8, w64, sums, mine, other, send, got, counts,
                    order_v, source_v, first_v, second_v, order_s, source_s,
                    lsem, tsem, qssem, qrsem, ssem, rsem, cssem, crsem, osem):
    slots = nodes * most
    lines = mask.shape[0]
    me, rep = lax.axis_index("tm"), lax.axis_index("rep")
    fetch = pltpu.make_async_copy(rows_hbm, rows, lsem.at[0])
    fetch.start()
    barrier = pltpu.get_barrier_semaphore()

    def hello(k, carry):
        pl.semaphore_signal(barrier, inc=1, device_id={"tm": lax.rem(me + k, nodes)})
        return carry

    lax.fori_loop(1, nodes, hello, 0)
    pl.semaphore_signal(barrier, inc=1, device_id={"rep": 1 - rep})

    upper = (iota((LANES, LANES), 0) <= iota((LANES, LANES), 1)).astype(f32).astype(bf16)
    both = jnp.concatenate([upper, jnp.ones((LANES, LANES), bf16)], axis=0)
    group = min(nodes, 16)
    size = group * lines
    r, c = iota((size, size), 0), iota((size, size), 1)
    earlier = ((r // lines == c // lines) & (c < r)).astype(f32).astype(bf16)
    live = mask[...] == 1
    livef = live.astype(f32)
    keys = key[...]

    def prefix(hits, lower):
        hits = hits.astype(bf16)
        above = dot(lower, hits).astype(bf16)
        return dot(jnp.concatenate([hits, above], axis=1), both)

    down = iota((LANES, LANES), 0)
    each = 4

    def invert(pieces, spot, values):
        first_v[...] = jnp.where(live, spot // LANES, -1)
        second_v[...] = spot % LANES
        piece_down = iota((pieces, LANES), 0)

        def some(q, total):
            for u in range(each):
                i = q * each + u
                high, low = values(i)
                hit = piece_down == first_v[pl.ds(i, 1), :]
                left = jnp.concatenate(
                    [jnp.where(hit, high, 0.0), jnp.where(hit, low, 0.0)], axis=0).astype(bf16)
                right = (down == second_v[pl.ds(i, 1), :]).astype(f32).astype(bf16)
                total = total + lax.dot_general(
                    left, right, (((1,), (1,)), ((), ())), preferred_element_type=f32)
            return total

        total = lax.fori_loop(0, lines // each, some, jnp.zeros((2 * pieces, LANES), f32))
        return (total[:pieces] * LANES + total[pieces:]).astype(i32)

    running = prefix(livef, earlier[:lines, :lines])
    place = running.astype(i32) - 1
    pieces = slots // LANES
    lanef = iota((1, LANES), 1).astype(f32)
    order_v[0:pieces, :] = within(invert(
        pieces, place, lambda i: (jnp.asarray(i, i32).astype(f32), lanef)), 0, lines * LANES - 1)
    order_v[pieces:pieces + 8, :] = within(jnp.broadcast_to(
        running[lines - 1:lines, LANES - 1:LANES], (8, LANES)).astype(i32), WINDOW, slots)
    list_copy = pltpu.make_async_copy(order_v, order_s, lsem.at[1])
    list_copy.start()
    list_copy.wait()
    fetch.wait()
    begin = order_s[pieces, 0] - WINDOW

    def take_tail(q, carry):
        for u in range(16):
            j = q * 16 + u
            g = begin + j
            tail[pl.ds(j, 1), :] = rows[pl.ds(order_s[g >> 7, g & (LANES - 1)], 1), :]
        return carry

    lax.fori_loop(0, WINDOW // 16, take_tail, 0)
    pl.semaphore_wait(barrier, nodes)
    ahead = pltpu.make_async_remote_copy(
        src_ref=tail, dst_ref=tailbuf, send_sem=tsem.at[0], recv_sem=tsem.at[1],
        device_id={"tm": lax.rem(me + 1, nodes)})
    ahead.start()

    slot = jnp.zeros((lines, LANES), f32)
    lane = iota((8, LANES), 1)
    parts = []
    for first in range(0, nodes, group):
        hits = [(live & (keys == b)).astype(f32) for b in range(first, first + group)]
        ranks = prefix(jnp.concatenate(hits, axis=0), earlier)
        for j, hit in enumerate(hits):
            b = first + j
            own = ranks[j * lines:(j + 1) * lines]
            slot = slot + hit * (own + (b * wide - 1.0))
            parts.append(jnp.where(lane == b % LANES, own[lines - 1:lines, LANES - 1:LANES], 0.0))
    counts[...] = sum(parts)
    back = slots - place
    packed[0:lines, :] = (back // LANES).astype(f32)
    packed[lines:2 * lines, :] = (back % LANES).astype(f32)
    source_v[...] = within(slots - invert(
        nodes * wide // LANES, slot.astype(i32),
        lambda i: (packed[pl.ds(i, 1), :], packed[pl.ds(lines + i, 1), :])), 0, slots)
    source_copy = pltpu.make_async_copy(source_v, source_s, lsem.at[2])
    source_copy.start()

    def count_copy(d, at):
        return pltpu.make_async_remote_copy(
            src_ref=counts, dst_ref=gotc.at[at], send_sem=cssem.at[d], recv_sem=crsem.at[at],
            device_id={"tm": d})

    def take(i, carry):
        def some(q, carry):
            for u in range(16):
                j = q * 16 + u
                packed[pl.ds(i * LANES + j, 1), :] = rows[pl.ds(order_s[i, j], 1), :]
            return carry
        return lax.fori_loop(0, LANES // 16, some, carry)

    lax.fori_loop(0, pieces, take, 0)

    def eight(x):
        x = x + pltpu.roll(x, 1, 0)
        x = x + pltpu.roll(x, 2, 0)
        x = x + pltpu.roll(x, 4, 0)
        return x[8:]

    def w8_own(c, carry):
        a = pl.multiple_of(c * STEP, STEP)
        w8[pl.ds(WINDOW + a, STEP), :] = eight(packed[pl.ds(a - 8, STEP + 8), :])
        return carry

    def stride_sum(ref, a, rows, stride):
        parts = [ref[pl.ds(a - stride * k, rows), :] for k in range(8)]
        while len(parts) > 1:
            parts = [parts[i] + parts[i + 1] for i in range(0, len(parts), 2)]
        return parts[0]

    def w64_at(c, carry):
        a = pl.multiple_of(c * STEP, STEP)
        w64[pl.ds(a, STEP), :] = stride_sum(w8, a, STEP, 8)
        return carry

    def w512_at(c, carry):
        a = pl.multiple_of(c * LANES, LANES)
        sums[pl.ds(a, LANES), :] = stride_sum(w64, WINDOW + a, LANES, 64)
        return carry

    own = WINDOW // STEP + 1
    last = (WINDOW + slots) // STEP
    lax.fori_loop(1, slots // STEP, w8_own, 0)
    lax.fori_loop(own + 1, last, w64_at, 0)
    lax.fori_loop(5, slots // LANES, w512_at, 0)
    ahead.wait()
    w8[0:STEP, :] = eight(jnp.concatenate([jnp.zeros((8, LANES), f32), tailbuf[0:STEP, :]], axis=0))
    for a in range(STEP, WINDOW, STEP):
        w8[a:a + STEP, :] = eight(tailbuf[a - 8:a + STEP, :])
    w8[WINDOW:WINDOW + STEP, :] = eight(
        jnp.concatenate([tailbuf[WINDOW - 8:WINDOW, :], packed[0:STEP, :]], axis=0))
    lax.fori_loop(1, own + 1, w64_at, 0)
    lax.fori_loop(0, 5, w512_at, 0)

    sums[pl.ds(slots, 8), :] = jnp.zeros((8, LANES), f32)

    def gather(ref, d):
        def some(q, carry):
            for u in range(8):
                j = q * 8 + u
                at = source_s[d * (wide // LANES) + q // (LANES // 8), q % (LANES // 8) * 8 + u]
                ref[d, pl.ds(j, 1), :] = sums[pl.ds(at, 1), :]
            return carry
        lax.fori_loop(0, most // 8, some, 0)

    def block_copy(d, at):
        return pltpu.make_async_remote_copy(
            src_ref=send.at[d], dst_ref=got.at[at], send_sem=ssem.at[d], recv_sem=rsem.at[at],
            device_id={"tm": d})

    half = nodes // 2
    near, far = me // half * half, (me // half + 1) % 2 * half
    seat = me % half

    def send_block(base, k):
        d = base + (seat + k) % half
        gather(send, d)
        block_copy(d, me).start()

    def swap_copy(s):
        return pltpu.make_async_remote_copy(
            src_ref=mine.at[s], dst_ref=other.at[s], send_sem=qssem.at[s], recv_sem=qrsem.at[s],
            device_id={"rep": 1 - rep})

    def out_copy(s):
        return pltpu.make_async_copy(got.at[s], out.at[s], osem.at[s])

    def squares(s):
        x = got[s]
        mine[s] = jnp.broadcast_to(jnp.sum(x * x, axis=1, keepdims=True), x.shape)
        swap_copy(s).start()

    gains = gain[...]

    def norm(s):
        swap_copy(s).wait()
        got[s] = got[s] * gains * lax.rsqrt((mine[s] + other[s]) / F + EPS)
        out_copy(s).start()

    def receive(base, k):
        s = base + (seat + half - k) % half
        block_copy(s, s).wait()
        squares(s)
        return s

    def loop(first, last, body, carry):
        return lax.fori_loop(first, last, body, carry)

    def send_both(k, carry):
        send_block(far, k)
        send_block(near, k)
        return carry

    source_copy.wait()
    send_block(far, 0)
    loop(1, half, send_both, 0)

    def send_counts(k, carry):
        count_copy(lax.rem(me + k, nodes), me).start()
        return carry

    loop(1, nodes, send_counts, 0)
    gotc[me] = counts[...]
    gather(got, me)
    squares(me)

    def get_both(k, carry):
        s = receive(far, k)
        norm(jnp.where(k == 1, far + seat, near + (seat + half - k + 1) % half))
        receive(near, k)
        norm(s)
        return carry

    receive(far, 0)
    norm(me)
    loop(1, half, get_both, 0)
    norm(near + (seat + 1) % half)

    def finish(k, carry):
        s = lax.rem(me + k, nodes)
        count_copy(s, s).wait()
        return carry

    loop(1, nodes, finish, 0)

    def left(s, carry):
        out_copy(s).wait()
        return carry

    loop(0, nodes, left, 0)


def place_kernel(nodes, most, got_hbm, gotc, out, got, starts_v, starts_s, gsem, sem):
    me = lax.axis_index("tm")

    def block(s):
        return pltpu.make_async_copy(got_hbm.at[s], got.at[s], gsem.at[s])

    def begin(s, carry):
        block(s).start()
        return carry

    lax.fori_loop(0, nodes, begin, 0)
    shape = (nodes, nodes * 8)
    before = (iota(shape, 1) % 8 == 0) & (iota(shape, 1) // 8 < iota(shape, 0))
    numbers = gotc[...].reshape(nodes * 8, LANES).astype(bf16)
    starts = dot(before.astype(f32).astype(bf16), numbers).astype(i32)
    starts_v[...] = within(starts, 0, (nodes - 1) * most)
    fetch = pltpu.make_async_copy(starts_v, starts_s, sem)
    fetch.start()
    out[...] = jnp.zeros_like(out)
    fetch.wait()

    def sender(s, carry):
        block(s).wait()
        out[pl.ds(starts_s[s, me], most), :] = got[s]
        return carry

    lax.fori_loop(0, nodes, sender, 0)


def local(nodes, rows, row_mask, key_bucket, gain):
    size_rows, half = rows.shape
    most = 3 * size_rows // (4 * nodes)
    slots = nodes * most
    lines = size_rows // LANES
    vm = pl.BlockSpec(memory_space=VMEM)
    hbm = pl.BlockSpec(memory_space=pl.ANY)
    wide = -(-most // LANES) * LANES
    dma = pltpu.SemaphoreType.DMA
    blocks = pltpu.VMEM((nodes, most, half), f32)
    edge = pltpu.VMEM((WINDOW, half), f32)
    table = pltpu.VMEM((lines, LANES), i32)
    order, source = (slots // LANES + 8, LANES), (nodes * wide // LANES, LANES)
    got, gotc = pl.pallas_call(
        functools.partial(exchange_kernel, nodes, most, wide),
        out_shape=(
            jax.ShapeDtypeStruct((nodes, most, half), f32),
            jax.ShapeDtypeStruct((nodes, 8, LANES), f32),
        ),
        in_specs=[hbm, vm, vm, vm],
        out_specs=(hbm, vm),
        scratch_shapes=[
            pltpu.VMEM((size_rows, half), f32),
            pltpu.VMEM((slots, half), f32),
            edge, edge,
            pltpu.VMEM((WINDOW + slots, half), f32),
            pltpu.VMEM((WINDOW + slots, half), f32),
            pltpu.VMEM((slots + 8, half), f32),
            blocks, blocks, blocks, blocks,
            pltpu.VMEM((8, LANES), f32),
            pltpu.VMEM(order, i32), pltpu.VMEM(source, i32),
            table, table,
            pltpu.SMEM(order, i32), pltpu.SMEM(source, i32),
            dma((3,)), dma((2,)),
        ] + [dma((nodes,))] * 7,
        compiler_params=pltpu.CompilerParams(collective_id=0, has_side_effects=True),
        name="exchange",
    )(rows, row_mask.reshape(lines, LANES), key_bucket.reshape(lines, LANES), gain.reshape(1, half))
    return pl.pallas_call(
        functools.partial(place_kernel, nodes, most),
        out_shape=jax.ShapeDtypeStruct((slots, half), f32),
        in_specs=[hbm, vm],
        out_specs=vm,
        scratch_shapes=[
            blocks,
            pltpu.VMEM((nodes, LANES), i32), pltpu.SMEM((nodes, LANES), i32),
            dma((nodes,)), dma,
        ],
        name="place",
    )(got, gotc)


def solution(mesh):
    in_specs = (P("tm", "rep"), P("tm"), P("tm"), P("rep"))
    body = functools.partial(local, mesh.shape["tm"])
    return jax.shard_map(body, mesh=mesh, in_specs=in_specs, out_specs=P("tm", "rep"), check_vma=False)
```
